32 devices in a mesh: group: 4 (over y, x), shard: 8 (over z, core).
Axes of the slice: x: 2, y: 2, z: 4, core: 2. Of those that a mesh axis runs over, the one named last changes fastest.
Arguments:
- embeddings: bfloat16 [128, 256, 768], P(('group', 'shard')), may hold values from -6 to 6
- assignments: int32 [128, 2, 256], P(('group', 'shard')), may hold values from 0 to 4095, as said below
- block_group: int32 [128], P(('group', 'shard')), may hold values from 0 to 3, as said below
- centroids: float32 [4, 4096, 768], P('group'), may hold values from -6 to 6
Outputs:
- subcentroids: float32 [4, 4096, 768], P('group', 'shard')
- inertia: float32 [4, 4096], P('group', 'shard')
The draws below stay inside these ranges and needn't reach their ends.
Inputs may be any that keep to these rules, and one draw needn't show every extreme that they name: `block_group`: of the 4 blocks of one device at most 2 name the same group; in every draw, for some group and some shard index, every device of that shard index has exactly 2 blocks naming that group. `assignments`: labels k with the same k // 512 form one range. In each block and iteration at most 64 rows have labels in one range; in every draw there is an iteration in which every block has exactly 64 rows in one common range.
All inputs are finite; a program needn't handle non-finite values.
Results may differ from the reference program's by a relative error of at most 0.0003.
Values may be sent and summed in bfloat16 or wider, within the bound.
A program may use at most 128 MiB of HBM per device.

```python
import jax
import jax.numpy as jnp

D = 768
K = 4096
BLOCK_ROWS = 256
ITERS = 2
BLK_DEV = 4
CAP = 2
BLOCKS = 128
MOST = 64
N_GROUP = 4
N_SHARD = 8


def draw_block_group(key, part):
    devices = BLOCKS // BLK_DEV
    pool_size = N_GROUP * CAP
    key_list = jax.random.split(jax.random.fold_in(key, 11), devices)
    ordering = jax.vmap(lambda subkey: jax.random.permutation(subkey, pool_size))(key_list)
    spread_out = (ordering[:, :BLK_DEV] % N_GROUP).astype(jnp.int32)
    rest_size = (N_GROUP - 1) * CAP
    key_other = jax.random.split(jax.random.fold_in(key, 12), devices)
    ordering_other = jax.vmap(lambda subkey: jax.random.permutation(subkey, rest_size))(key_other)
    target = jax.random.randint(jax.random.fold_in(key, 13), (), 0, N_GROUP).astype(jnp.int32)
    column = jax.random.randint(jax.random.fold_in(key, 14), (), 0, N_SHARD).astype(jnp.int32)
    others = ((target + 1 + ordering_other[:, :BLK_DEV - CAP] % (N_GROUP - 1)) % N_GROUP).astype(jnp.int32)
    crowded = jnp.concatenate([jnp.full((devices, CAP), target, jnp.int32), others], axis=1)
    chosen = jnp.arange(devices) % N_SHARD == column
    routing = jnp.where(chosen[:, None], crowded, spread_out)
    return routing.reshape(-1).astype(jnp.int32)


def draw_assignments(key, part):
    owned = K // N_SHARD
    cells = BLOCKS * ITERS
    pool_size = N_SHARD * MOST
    key_list = jax.random.split(jax.random.fold_in(key, 21), cells)
    spread_out = jax.vmap(lambda subkey: jax.random.permutation(subkey, pool_size)[:BLOCK_ROWS] % N_SHARD)(key_list)
    rest_size = (N_SHARD - 1) * MOST
    key_other = jax.random.split(jax.random.fold_in(key, 22), cells)
    other_part = jax.vmap(lambda subkey: jax.random.permutation(subkey, rest_size)[:BLOCK_ROWS - MOST] % (N_SHARD - 1))(key_other)
    target = jax.random.randint(jax.random.fold_in(key, 23), (), 0, N_SHARD).astype(jnp.int32)
    crowded = jnp.concatenate([jnp.full((cells, MOST), target, jnp.int32), ((target + 1 + other_part) % N_SHARD).astype(jnp.int32)], axis=1)
    key_mix = jax.random.split(jax.random.fold_in(key, 24), cells)
    crowded = jax.vmap(lambda subkey, row: row[jax.random.permutation(subkey, BLOCK_ROWS)])(key_mix, crowded)
    busy = jax.random.randint(jax.random.fold_in(key, 25), (), 0, ITERS).astype(jnp.int32)
    is_busy = jnp.arange(cells) % ITERS == busy
    range_ids = jnp.where(is_busy[:, None], crowded, spread_out).astype(jnp.int32)
    offsets = jax.random.randint(jax.random.fold_in(key, 26), (cells, BLOCK_ROWS), 0, owned).astype(jnp.int32)
    labels = range_ids * owned + offsets
    return labels.reshape(BLOCKS, ITERS, BLOCK_ROWS).astype(jnp.int32)


def steps_of(stream_key, shape, cuts, least, high):
    loudness, own = 1.0, jax.random.fold_in(stream_key, 6)
    for dim, parts in cuts:
        heights = jnp.exp(jax.random.uniform(jax.random.fold_in(own, dim), (parts,), jnp.float32, least / len(cuts), high / len(cuts)))
        loudness = loudness * jnp.repeat(heights, shape[dim] // parts).reshape([-1 if axis == dim else 1 for axis in range(len(shape))])
    return loudness


def normal_values(stream_key, extent, width, reach, cuts=(), held_as=jnp.bfloat16):
    level = steps_of(stream_key, extent, cuts, -0.22, 0.18) if cuts else 1.0
    entries = jax.random.normal(stream_key, extent, jnp.float32) * width * level
    return jnp.minimum(jnp.maximum(entries, -reach), reach).astype(held_as)


def setup_inputs(seed: int = 0) -> dict:
    arg_keys = jax.random.split(jax.random.key(seed), 5)
    embeddings = normal_values(arg_keys[0], (BLOCKS, BLOCK_ROWS, D), 1.0, 6.0, ((0, 32),))
    assignments = draw_assignments(jax.random.fold_in(arg_keys[4], 71), 0)
    block_group = draw_block_group(jax.random.fold_in(arg_keys[4], 71), 0)
    centroids = normal_values(arg_keys[3], (N_GROUP, K, D), 1.0, 6.0, ((0, 4),), jnp.float32)
    return dict(embeddings=embeddings, assignments=assignments, block_group=block_group, centroids=centroids)


PRIOR = 8.0


def reference(embeddings, assignments, block_group, centroids):
    block_count, block_rows, features = embeddings.shape
    groups, centers, unused = centroids.shape
    flat_rows = embeddings.reshape(-1, features).astype(jnp.float32)
    owners = jnp.repeat(block_group, block_rows).astype(jnp.int32)
    previous = centroids.reshape(groups * centers, features)
    inertia = jnp.zeros((groups * centers,), jnp.float32)
    for iteration in range(ITERS):
        labels = assignments[:, iteration, :].reshape(-1).astype(jnp.int32)
        segment = owners * centers + labels
        center_sums = jax.ops.segment_sum(flat_rows, segment, num_segments=groups * centers)
        counts = jax.ops.segment_sum(jnp.ones(labels.shape, jnp.float32), segment, num_segments=groups * centers)
        if iteration == ITERS - 1:
            difference = flat_rows - previous[segment]
            per_row = jnp.sum(difference * difference, axis=1)
            within = jax.ops.segment_sum(per_row, segment, num_segments=groups * centers)
            inertia = within / ((counts + PRIOR) * features)
        previous = (center_sums + PRIOR * previous) / (counts + PRIOR)[:, None]
    return previous.reshape(groups, centers, features), inertia.reshape(groups, centers)
```

```python
import functools

import jax
import jax.numpy as jnp
from jax import lax
from jax.experimental import pallas as pl
from jax.experimental.pallas import tpu as pltpu
from jax.sharding import PartitionSpec as P

PRIOR = 8.0
META = 8
CHUNKS = 3
MESH = pl.DeviceIdType.MESH


def exchange_kernel(n_gather, n_swap, width, column, *refs):
    n_in = n_gather + n_swap
    gathers, swaps = refs[:n_gather], refs[n_gather:n_in]
    outs = refs[n_in : 2 * n_in]
    gather_outs, swap_outs = outs[:n_gather], outs[n_gather:]
    scratch = refs[2 * n_in :]
    stages = scratch[:n_gather]
    scratch = scratch[n_gather:]

    groups, shards = lax.axis_size("group"), lax.axis_size("shard")
    chips = shards // 2
    mine, place = lax.axis_index("group"), lax.axis_index("shard")
    chip, core = place // 2, place % 2
    partner = (mine, chip * 2 + 1 - core)
    right = (mine, lax.rem(chip + 1, chips) * 2 + core)
    left = (mine, lax.rem(chip + chips - 1, chips) * 2 + core)

    def peer(step):
        return lax.rem(mine + step, groups)

    barrier = pltpu.get_barrier_semaphore()
    greeted = 0
    if n_gather:
        for device in (left, right, partner):
            pl.semaphore_signal(barrier, inc=1, device_id=device, device_id_type=MESH)
        greeted += 3
    if n_swap:
        for step in range(1, groups):
            pl.semaphore_signal(
                barrier, inc=1, device_id=(peer(step), place), device_id_type=MESH
            )
        greeted += groups - 1

    loads = []
    if n_gather:
        load_sem = scratch[0]
        for i in range(n_gather):
            source = gathers[i]
            if i == 0:
                source = source.at[:, :, pl.ds(column, width)]
            load = pltpu.make_async_copy(source, stages[i], load_sem.at[i])
            load.start()
            loads.append(load)
    pl.semaphore_wait(barrier, greeted)

    swap_copies = []
    if n_swap:
        swap_send, swap_recv = scratch[-2:]
        for step in range(1, groups):
            for i in range(n_swap):
                copy = pltpu.make_async_remote_copy(
                    src_ref=swaps[i].at[peer(step)],
                    dst_ref=swap_outs[i].at[step - 1],
                    send_sem=swap_send.at[i, step - 1],
                    recv_sem=swap_recv.at[i, step - 1],
                    device_id=(peer(step), place),
                    device_id_type=MESH,
                )
                copy.start()
                swap_copies.append(copy)

    if n_gather:
        store_sem, send_r, recv_r, send_l, recv_l, send_p, recv_p = scratch[1:8]
        stores = []

        def hop(i, source, origin, step, to, sends, recvs):
            return pltpu.make_async_remote_copy(
                src_ref=source,
                dst_ref=gather_outs[i].at[origin * 2 + core],
                send_sem=sends.at[i, step],
                recv_sem=recvs.at[i, step],
                device_id=to,
                device_id_type=MESH,
            )

        for i in range(n_gather):
            loads[i].wait()
            store = pltpu.make_async_copy(
                stages[i], gather_outs[i].at[place], store_sem.at[i]
            )

            @pl.when(chip < chips - 1)
            def _():
                hop(i, stages[i], chip, 0, right, send_r, recv_r).start()

            @pl.when(chip > 0)
            def _():
                hop(i, stages[i], chip, 0, left, send_l, recv_l).start()

            hop(i, stages[i], chip, chip, partner, send_p, recv_p).start()
            store.start()
            stores.append(store)

        for step in range(chips - 1):
            for i in range(n_gather):
                from_left = chip - 1 - step

                @pl.when(from_left >= 0)
                def _():
                    block = gather_outs[i].at[from_left * 2 + core]
                    hop(i, block, from_left, step, right, send_r, recv_r).wait_recv()

                    if step < chips - 2:

                        @pl.when(chip < chips - 1)
                        def _():
                            hop(i, block, from_left, step + 1, right, send_r, recv_r).start()

                    hop(i, block, from_left, from_left, partner, send_p, recv_p).start()

                from_right = chip + 1 + step

                @pl.when(from_right <= chips - 1)
                def _():
                    block = gather_outs[i].at[from_right * 2 + core]
                    hop(i, block, from_right, step, left, send_l, recv_l).wait_recv()

                    if step < chips - 2:

                        @pl.when(chip > 0)
                        def _():
                            hop(i, block, from_right, step + 1, left, send_l, recv_l).start()

                    hop(i, block, from_right, from_right, partner, send_p, recv_p).start()

        for i in range(n_gather):
            stores[i].wait()
            for step in range(chips - 1):

                @pl.when((chip - step >= 0) & (chip < chips - 1))
                def _():
                    hop(i, stages[i], chip, step, right, send_r, recv_r).wait_send()

                @pl.when((chip + step <= chips - 1) & (chip > 0))
                def _():
                    hop(i, stages[i], chip, step, left, send_l, recv_l).wait_send()

            for origin in range(chips):
                hop(i, stages[i], origin, origin, partner, send_p, recv_p).wait()

    for copy in swap_copies:
        copy.wait()


def exchange(gathers, swaps, width, column, key):
    groups, shards = lax.axis_size("group"), lax.axis_size("shard")
    chips = shards // 2
    n_gather, n_swap = len(gathers), len(swaps)
    shapes, scratch = [], []
    for i, array in enumerate(gathers):
        block = array.shape[:-1] + (width if i == 0 else array.shape[-1],)
        shapes.append(jax.ShapeDtypeStruct((shards,) + block, array.dtype))
        scratch.append(pltpu.VMEM(block, array.dtype))
    for array in swaps:
        shapes.append(jax.ShapeDtypeStruct((groups - 1,) + array.shape[1:], array.dtype))
    dma = pltpu.SemaphoreType.DMA
    if n_gather:
        scratch += [dma((n_gather,)), dma((n_gather,))]
        scratch += [dma((n_gather, max(chips - 1, 1)))] * 4
        scratch += [dma((n_gather, chips))] * 2
    if n_swap:
        scratch += [dma((n_swap, groups - 1))] * 2
    return pl.pallas_call(
        functools.partial(exchange_kernel, n_gather, n_swap, width, column),
        out_shape=shapes,
        in_specs=[pl.BlockSpec(memory_space=pl.ANY)] * (n_gather + n_swap),
        out_specs=[pl.BlockSpec(memory_space=pl.ANY)] * (n_gather + n_swap),
        scratch_shapes=scratch,
        compiler_params=pltpu.CompilerParams(collective_id=key, has_side_effects=True),
    )(*gathers, *swaps)


def tally_kernel(per_step, iters, with_extra, owners, labels, extra, rows, sums, *more):
    step = pl.program_id(0)
    centers = sums.shape[2]
    block_rows = rows.shape[1]

    @pl.when(step == 0)
    def _():
        sums[...] = jnp.zeros_like(sums)
        if with_extra:
            more[0][...] = jnp.zeros_like(more[0])

    ids = lax.broadcasted_iota(jnp.int32, (centers, block_rows), 0)
    for block in range(per_step):
        owner = owners[step * per_step + block]
        for t in range(iters):
            onehot = (ids == labels[block, t : t + 1, :]).astype(jnp.bfloat16)
            sums[owner, t] += jnp.dot(
                onehot, rows[block], preferred_element_type=jnp.float32
            )
            if with_extra:
                more[0][owner, t] += lax.dot_general(
                    extra[block],
                    onehot,
                    (((1,), (1,)), ((), ())),
                    preferred_element_type=jnp.float32,
                )


def tally(owners, labels, extra, rows, groups, centers, per_step, with_extra):
    blocks, iters, block_rows = labels.shape
    width = rows.shape[-1]
    shapes = [jax.ShapeDtypeStruct((groups, iters, centers, width), jnp.float32)]
    if with_extra:
        shapes.append(jax.ShapeDtypeStruct((groups, iters, extra.shape[1], centers), jnp.float32))
    out_specs = [pl.BlockSpec(s.shape, lambda i, o: (0, 0, 0, 0)) for s in shapes]
    return pl.pallas_call(
        functools.partial(tally_kernel, per_step, iters, with_extra),
        out_shape=shapes,
        grid_spec=pltpu.PrefetchScalarGridSpec(
            num_scalar_prefetch=1,
            grid=(blocks // per_step,),
            in_specs=[
                pl.BlockSpec((per_step, iters, block_rows), lambda i, o: (i, 0, 0)),
                pl.BlockSpec((per_step,) + extra.shape[1:], lambda i, o: (i, 0, 0)),
                pl.BlockSpec((per_step, block_rows, width), lambda i, o: (i, 0, 0)),
            ],
            out_specs=out_specs,
        ),
        compiler_params=pltpu.CompilerParams(vmem_limit_bytes=48 * 2**20),
    )(owners, labels, extra, rows)


def body(embeddings, assignments, block_group, centroids):
    groups, shards = lax.axis_size("group"), lax.axis_size("shard")
    mine, place = lax.axis_index("group"), lax.axis_index("shard")
    local, block_rows, features = embeddings.shape
    iters = assignments.shape[1]
    owned = centroids.shape[1] // shards
    chunks = CHUNKS if features % (CHUNKS * 128) == 0 else 1
    width = features // chunks
    blocks = shards * local

    wide = embeddings.astype(jnp.float32)
    squares = jnp.sum(wide * wide, axis=2)
    meta = jnp.concatenate(
        [
            assignments.astype(jnp.float32),
            jnp.broadcast_to(
                block_group[:, None, None].astype(jnp.float32), (local, 1, block_rows)
            ),
            squares[:, None, :],
            jnp.zeros((local, META - iters - 2, block_rows), jnp.float32),
        ],
        axis=1,
    )

    rows, metas = exchange([embeddings, meta], [], width, 0, 0)
    metas = metas.reshape(blocks, META, block_rows)
    labels = metas[:, :iters].astype(jnp.int32) - place * owned
    owners = metas[:, iters, 0].astype(jnp.int32)
    square = metas[:, iters + 1]
    high = lax.reduce_precision(square, 8, 7)
    middle = lax.reduce_precision(square - high, 8, 7)
    low = square - high - middle
    one = jnp.ones_like(square)
    zero = jnp.zeros_like(square)
    extra = jnp.stack([one, high, middle, low] + [zero] * 12, axis=1).astype(jnp.bfloat16)

    totals = []
    tail = None
    pending = []
    for chunk in range(chunks):
        result = tally(
            owners,
            labels,
            extra,
            rows.reshape(blocks, block_rows, width),
            groups,
            owned,
            local,
            chunk == 0,
        )
        column = (chunk + 1) * width
        if chunk + 1 < chunks:
            rows, *got = exchange([embeddings], result, width, column, chunk + 1)
        else:
            got = exchange([], result, width, 0, chunk + 1)
        whole = [
            lax.dynamic_index_in_dim(kept, mine, 0, keepdims=False) + jnp.sum(came, axis=0)
            for kept, came in zip(result, got)
        ]
        totals.append(whole[0])
        if chunk == 0:
            tail = whole[1]

    prior = lax.dynamic_slice_in_dim(centroids[0], place * owned, owned, 0)
    counts = tail[:, 0]
    within = tail[iters - 1, 1] + tail[iters - 1, 2] + tail[iters - 1, 3]
    pieces = []
    for chunk in range(chunks):
        previous = prior[:, chunk * width : (chunk + 1) * width]
        for t in range(iters):
            sums = totals[chunk][t]
            count = counts[t][:, None]
            if t == iters - 1:
                within = within + jnp.sum(
                    previous * (count * previous - 2.0 * sums), axis=1
                )
            previous = (sums + PRIOR * previous) / (count + PRIOR)
        pieces.append(previous)
    inertia = within / ((counts[iters - 1] + PRIOR) * features)
    return (jnp.concatenate(pieces, axis=1)[None], inertia[None])


def solution(mesh):
    in_specs = (
        P(("group", "shard"), None, None),
        P(("group", "shard"), None, None),
        P(("group", "shard")),
        P("group", None, None),
    )
    out_specs = (P("group", "shard", None), P("group", "shard"))
    return jax.shard_map(body, mesh=mesh, in_specs=in_specs, out_specs=out_specs, check_vma=False)
```
